32 devices in a mesh: dp: 4 (over x, core), mp: 8 (over z, y).
Axes of the slice: x: 2, y: 2, z: 4, core: 2. Of those that a mesh axis runs over, the one named last changes fastest.
Arguments:
- tokens: bfloat16 [1280, 1792], P(('dp', 'mp')), may hold values from -6 to 6
- norm_gain: float32 [1792], replicated, may hold values from 0.5 to 1.5
- norm_bias: float32 [1792], replicated, may hold values from -3 to 3
- w_in: bfloat16 [1792, 15360], P('dp', 'mp'), may hold values from -0.125 to 0.125
- b_in: float32 [15360], P('mp'), may hold values from -3 to 3
- w_out: bfloat16 [15360, 1792], P('mp', 'dp'), may hold values from -0.046875 to 0.046875
- b_out: float32 [1792], replicated, may hold values from -3 to 3
Outputs:
- result: bfloat16 [1280, 1792], P(('dp', 'mp'))
The draws below stay inside these ranges and needn't reach their ends.
All inputs are finite; a program needn't handle non-finite values.
Results may differ from the reference program's by a relative error of at most 0.0042.
Values may be sent and summed in bfloat16 or wider, within the bound.
A program may use at most 128 MiB of HBM per device.

```python
import jax
import jax.numpy as jnp
from jax import lax

D = 1792
FF = 15360
TOK_DEV = 40
TOKENS = 1280
N_MP = 8


def block_scale(rng, dims, pieces, low, top_value):
    level, own = 1.0, jax.random.fold_in(rng, 6)
    for axis_at, shards_of in pieces:
        draws = jnp.exp(jax.random.uniform(jax.random.fold_in(own, axis_at), (shards_of,), jnp.float32, low / len(pieces), top_value / len(pieces)))
        level = level * jnp.repeat(draws, dims[axis_at] // shards_of).reshape([-1 if axis == axis_at else 1 for axis in range(len(dims))])
    return level


def scatter_about(own_key, extent, scale, limit, split=(), dtype=jnp.bfloat16):
    array = scale * jax.random.normal(own_key, extent, jnp.float32)
    if split:
        array = array * block_scale(own_key, extent, split, -0.22, 0.18)
    return jnp.clip(array, -limit, limit).astype(dtype)


def setup_inputs(seed: int = 0) -> dict:
    streams_of = jax.random.split(jax.random.key(seed), 8)
    return {
        "tokens": scatter_about(streams_of[0], (TOKENS, D), 1.0, 6.0, ((0, 32),)),
        "norm_gain": jnp.clip(jax.random.uniform(streams_of[1], (D,), jnp.float32, 0.5, 1.5), 0.5, 1.5),
        "norm_bias": scatter_about(streams_of[2], (D,), 0.5, 3.0, (), jnp.float32),
        "w_in": scatter_about(streams_of[3], (D, FF), D ** -0.5, 0.125, ((0, 4), (1, 8))),
        "b_in": scatter_about(streams_of[4], (FF,), 0.5, 3.0, ((0, 8),), jnp.float32),
        "w_out": scatter_about(streams_of[5], (FF, D), FF ** -0.5, 0.046875, ((0, 8), (1, 4))),
        "b_out": scatter_about(streams_of[6], (D,), 0.5, 3.0, (), jnp.float32),
    }


def block_rows(rows, norm_gain, norm_bias, w_in, b_in, w_out, b_out):
    values = rows.astype(jnp.float32)
    center = lax.optimization_barrier(jnp.mean(values, axis=1, keepdims=True))
    spread = lax.optimization_barrier(jnp.mean((values - center) ** 2, axis=1, keepdims=True))
    normed = ((values - center) / jnp.sqrt(spread + 1e-06) * norm_gain + norm_bias).astype(jnp.bfloat16)
    pre = jnp.dot(normed, w_in, preferred_element_type=jnp.float32) + b_in
    hidden = jax.nn.gelu(pre, approximate=False).astype(jnp.bfloat16)
    summed = jnp.dot(hidden, w_out, preferred_element_type=jnp.float32)
    return (values + summed + b_out).astype(jnp.bfloat16)

def reference(tokens, norm_gain, norm_bias, w_in, b_in, w_out, b_out):
    group = TOK_DEV * N_MP
    blocks = tokens.reshape(TOKENS // group, group, D)
    done = lax.map(lambda rows: block_rows(rows, norm_gain, norm_bias, w_in, b_in, w_out, b_out), blocks)
    return done.reshape(TOKENS, D)
```

```python
import functools

import jax
import jax.numpy as jnp
from jax import lax
from jax.experimental import pallas as pl
from jax.experimental.pallas import tpu as pltpu
from jax.sharding import PartitionSpec as P

MESH = pl.DeviceIdType.MESH
LANES = 128
VMEM_GRANT = 60 * 2**20


def flip(index, mask, size):
    out, bit = index, 1
    while bit < size:
        if mask & bit:
            out = out + bit - 2 * bit * (lax.rem(lax.div(index, bit), 2))
        bit *= 2
    return out


def gelu(pre):
    return 0.5 * pre * (1.0 + lax.erf(pre * (0.5**0.5)))


def kernel(
    lines, tokens, gain, bias, w_in, b_in, w_out, b_out, out,
    shift, tok, win, wout, normed, hidden, part, own, from_y, sums, from_z, to_x, kept, from_x,
    tok_sem, win_sem, wout_sem, y_sem, z_sem, x_sem, local_sem, send_sem,
):
    dp, mp = lax.axis_index("dp"), lax.axis_index("mp")
    x, core = lax.div(dp, 2), lax.rem(dp, 2)
    z, y = lax.div(mp, 2), lax.rem(mp, 2)
    ox, oy = 1 - x, 1 - y
    rows, depth = tokens.shape[0], w_in.shape[0]
    units = w_in.shape[1]
    half = units // 2
    start = half // LANES * LANES
    width = units - start
    x_dev = (2 * ox + core, mp)
    core_dev = (2 * x + 1 - core, mp)
    y_dev = (dp, 2 * z + oy)
    z_at = [flip(z, k, lines) for k in range(lines)]
    z_dev = [(dp, 2 * z_at[k] + y) for k in range(lines)]

    barrier = pltpu.get_barrier_semaphore()
    partners = [x_dev, core_dev, y_dev] + z_dev[1:]
    for partner in partners:
        pl.semaphore_signal(barrier, inc=1, device_id=partner, device_id_type=MESH)
    pl.semaphore_wait(barrier, len(partners))

    sends = []

    def send(src, dst, sem, device):
        copy = pltpu.make_async_remote_copy(
            src_ref=src, dst_ref=dst, send_sem=send_sem.at[len(sends)], recv_sem=sem,
            device_id=device, device_id_type=MESH,
        )
        copy.start()
        sends.append(copy)

    def arrive(dst, sem):
        pltpu.make_async_remote_copy(
            src_ref=dst, dst_ref=dst, send_sem=send_sem.at[0], recv_sem=sem,
            device_id=x_dev, device_id_type=MESH,
        ).wait_recv()

    def slot(yy, zz, side):
        return (yy * lines + zz) * 2 + side

    mine = tok.at[slot(y, z, x)]
    mine_sem = tok_sem.at[y, z, x]
    send(tokens, mine, mine_sem, x_dev)
    for k in range(1, lines):
        send(tokens, mine, mine_sem, z_dev[k])
    send(tokens, mine, mine_sem, y_dev)
    locals_ = [pltpu.make_async_copy(tokens, mine, local_sem.at[0])]

    def columns(weight, side):
        return weight.at[:, pl.ds(pl.multiple_of(side * start, LANES), width)]


    def rows_of(full, owner):
        return full.at[pl.ds(pl.multiple_of(owner * depth, 16), depth), :]

    far, near, across = 2 * ox + core, 2 * x + 1 - core, 2 * ox + 1 - core
    send(columns(w_in, ox), rows_of(win, dp), win_sem.at[dp], x_dev)
    send(columns(w_in, x), rows_of(win, dp), win_sem.at[dp], core_dev)
    send(columns(w_out, ox), rows_of(wout, dp), wout_sem.at[dp], x_dev)
    send(columns(w_out, x), rows_of(wout, dp), wout_sem.at[dp], core_dev)
    locals_.append(pltpu.make_async_copy(columns(w_in, x), rows_of(win, dp), local_sem.at[1]))
    locals_.append(pltpu.make_async_copy(columns(w_out, x), rows_of(wout, dp), local_sem.at[2]))
    for copy in locals_:
        copy.start()

    shift[...] = jnp.broadcast_to(b_in[...], shift.shape)

    arrive(tok.at[slot(y, z, ox)], tok_sem.at[y, z, ox])
    for k in range(1, lines):
        send(tok.at[slot(y, z, ox)], tok.at[slot(y, z, ox)], tok_sem.at[y, z, ox], z_dev[k])
    send(tok.at[slot(y, z, ox)], tok.at[slot(y, z, ox)], tok_sem.at[y, z, ox], y_dev)
    for side in (x, ox):
        for k in range(1, lines):
            block, sem = tok.at[slot(y, z_at[k], side)], tok_sem.at[y, z_at[k], side]
            arrive(block, sem)
            send(block, block, sem, y_dev)

    def normalise(yy, zz):
        pair = jnp.concatenate(
            [tok[slot(yy, zz, 0)].astype(jnp.float32), tok[slot(yy, zz, 1)].astype(jnp.float32)], axis=0
        )
        center = jnp.mean(pair, axis=1, keepdims=True)
        spread = jnp.mean((pair - center) ** 2, axis=1, keepdims=True)
        value = (pair - center) / jnp.sqrt(spread + 1e-06) * gain[...] + bias[...]
        normed[yy, pl.ds(pl.multiple_of(zz * 2 * rows, 16), 2 * rows), :] = value.astype(
            normed.dtype
        )

    tile = 2 * LANES if width % (2 * LANES) == 0 else LANES

    def first(yy):
        def step(n, carry):
            at = pl.ds(pl.multiple_of(n * tile, LANES), tile)
            pre = jnp.dot(normed[yy], win[:, at], preferred_element_type=jnp.float32)
            pre = pre + shift[:1, pl.ds(pl.multiple_of(x * start + n * tile, LANES), tile)]
            unit = x * start + n * tile + lax.broadcasted_iota(jnp.int32, pre.shape, 1)
            keep = (unit >= x * half) & (unit < (x + 1) * half)
            hidden[yy, :, at] = jnp.where(keep, gelu(pre), 0.0).astype(hidden.dtype)
            return carry

        lax.fori_loop(0, width // tile, step, 0)

    locals_[0].wait()

    def norm_own(zz, carry):
        normalise(y, zz)
        return carry

    lax.fori_loop(0, lines, norm_own, 0)

    arrive(rows_of(win, far), win_sem.at[far])
    send(rows_of(win, far), rows_of(win, far), win_sem.at[far], core_dev)
    locals_[1].wait()
    arrive(rows_of(win, near), win_sem.at[near])
    arrive(rows_of(win, across), win_sem.at[across])
    first(y)

    for k in range(lines):
        for side in (x, ox):
            arrive(tok.at[slot(oy, z_at[k], side)], tok_sem.at[oy, z_at[k], side])
        normalise(oy, z_at[k])
    first(oy)

    def second(q, yy, zz):
        side = x if q == 0 else ox
        act = hidden[yy, pl.ds(pl.multiple_of(zz * 2 * rows, 16), 2 * rows), :]
        weight = wout[pl.ds(pl.multiple_of(side * 2 * depth, 16), 2 * depth), :]
        return lax.dot_general(
            act, weight, (((1,), (1,)), ((), ())), preferred_element_type=jnp.float32
        )

    def product(q):
        for k in range(lines):
            part[q, z_at[k]] = second(q, oy, z_at[k]).astype(part.dtype)
            send(part.at[q, z_at[k]], from_y.at[q, z_at[k]], y_sem.at[q, z_at[k]], y_dev)

        def step(zz, carry):
            own[q, zz] = second(q, y, zz)
            return carry

        lax.fori_loop(0, lines, step, 0)

    def along_z(q):
        for k in list(range(1, lines)) + [0]:
            at = z_at[k]
            arrive(from_y.at[q, at], y_sem.at[q, at])
            total = own[q, at] + from_y[q, at].astype(jnp.float32)
            if k:
                sums[q, at] = total.astype(sums.dtype)
                send(sums.at[q, at], from_z.at[q, z], z_sem.at[q, z], z_dev[k])
            else:
                own[q, at] = total

    def along_x(q):
        side = x if q == 0 else ox
        total = own[q, z]
        for k in range(1, lines):
            arrive(from_z.at[q, z_at[k]], z_sem.at[q, z_at[k]])
            total = total + from_z[q, z_at[k]].astype(jnp.float32)
        own[q, z] = total
        to_x[q] = own[q, z, pl.ds(pl.multiple_of(ox * rows, 8), rows), :].astype(to_x.dtype)
        send(to_x.at[q], from_x.at[side], x_sem.at[side], x_dev)
        kept[side] = own[q, z, pl.ds(pl.multiple_of(x * rows, 8), rows), :]

    locals_[2].wait()
    arrive(rows_of(wout, near), wout_sem.at[near])
    product(0)
    arrive(rows_of(wout, far), wout_sem.at[far])
    send(rows_of(wout, far), rows_of(wout, far), wout_sem.at[far], core_dev)
    along_z(0)
    arrive(rows_of(wout, across), wout_sem.at[across])
    product(1)
    along_x(0)
    along_z(1)
    along_x(1)
    columns_of, added = 2 * depth, b_out[...]
    for side in range(2):
        at = slice(side * columns_of, (side + 1) * columns_of)
        arrive(from_x.at[side], x_sem.at[side])
        total = kept[side] + from_x[side].astype(jnp.float32)
        out[:, at] = tok[slot(y, z, x), :, at].astype(jnp.float32) + total + added[:, at]
    for copy in sends:
        copy.wait_send()


def fused(mp, tokens, gain, bias, w_in, b_in, w_out, b_out):
    rows, dim = tokens.shape
    depth, units = w_in.shape
    lines = mp // 2
    width = units - units // 2 // LANES * LANES
    columns = 2 * depth
    bf16, f32, dma = jnp.bfloat16, jnp.float32, pltpu.SemaphoreType.DMA
    vmem = pl.BlockSpec(memory_space=pltpu.VMEM)
    hbm = pl.BlockSpec(memory_space=pl.ANY)
    n_sends = (lines + 1) * 2 + 4 + 2 * (lines - 1) + 2 + 2 * (lines + lines - 1 + 1)
    return pl.pallas_call(
        functools.partial(kernel, lines),
        out_shape=jax.ShapeDtypeStruct((rows, dim), f32),
        in_specs=[hbm, vmem, vmem, hbm, vmem, hbm, vmem],
        out_specs=vmem,
        scratch_shapes=[
            pltpu.VMEM((8, units), f32),
            pltpu.VMEM((4 * lines + 1, rows, dim), bf16),
            pltpu.VMEM((dim, width), bf16),
            pltpu.VMEM((dim, width), bf16),
            pltpu.VMEM((2, lines * 2 * rows, dim), bf16),
            pltpu.VMEM((2, lines * 2 * rows, width), bf16),
            pltpu.VMEM((2, lines, 2 * rows, columns), bf16),
            pltpu.VMEM((2, lines, 2 * rows, columns), f32),
            pltpu.VMEM((2, lines, 2 * rows, columns), bf16),
            pltpu.VMEM((2, lines, 2 * rows, columns), bf16),
            pltpu.VMEM((2, lines, 2 * rows, columns), bf16),
            pltpu.VMEM((3, rows, columns), bf16),
            pltpu.VMEM((2, rows, columns), f32),
            pltpu.VMEM((3, rows, columns), bf16),
            dma((2, lines, 2)),
            dma((4,)),
            dma((4,)),
            dma((2, lines)),
            dma((2, lines)),
            dma((2,)),
            dma((3,)),
            dma((n_sends,)),
        ],
        compiler_params=pltpu.CompilerParams(
            collective_id=0, has_side_effects=True, vmem_limit_bytes=VMEM_GRANT
        ),
    )(tokens, gain[None], bias[None], w_in, b_in[None], w_out.T, b_out[None]).astype(bf16)


def gathered(tokens, norm_gain, norm_bias, w_in, b_in, w_out, b_out):
    values = tokens.astype(jnp.float32)
    center = jnp.mean(values, axis=1, keepdims=True)
    spread = jnp.mean((values - center) ** 2, axis=1, keepdims=True)
    normed = ((values - center) / jnp.sqrt(spread + 1e-06) * norm_gain + norm_bias).astype(
        jnp.bfloat16
    )
    w_in_full = lax.all_gather(w_in, "dp", axis=0, tiled=True)
    everyone = lax.all_gather(normed, "mp", axis=0, tiled=True)
    pre = jnp.dot(everyone, w_in_full, preferred_element_type=jnp.float32) + b_in
    hidden = jax.nn.gelu(pre, approximate=False).astype(jnp.bfloat16)
    w_out_full = lax.all_gather(w_out, "dp", axis=1, tiled=True)
    summed = lax.psum_scatter(
        jnp.dot(hidden, w_out_full, preferred_element_type=jnp.float32),
        "mp",
        scatter_dimension=0,
        tiled=True,
    )
    return (values + summed + b_out).astype(jnp.bfloat16)


def on_device(dp, mp, tokens, norm_gain, norm_bias, w_in, b_in, w_out, b_out):
    rows, (depth, units) = tokens.shape[0], w_in.shape
    fits = (
        dp == 4
        and mp % 2 == 0
        and mp & (mp - 1) == 0
        and units % LANES == 0
        and depth % 16 == 0
        and 2 * depth % LANES == 0
        and rows % 8 == 0
        and mp * 2 * rows * (2 * depth) * 2 * 24 < VMEM_GRANT
    )
    if fits:
        return fused(mp, tokens, norm_gain, norm_bias, w_in, b_in, w_out, b_out)
    return gathered(tokens, norm_gain, norm_bias, w_in, b_in, w_out, b_out)


def solution(mesh):
    placed = (P(("dp", "mp"), None), P(), P(), P("dp", "mp"), P("mp"), P("mp", "dp"), P())
    return jax.shard_map(
        functools.partial(on_device, mesh.shape["dp"], mesh.shape["mp"]),
        mesh=mesh,
        in_specs=placed,
        out_specs=P(("dp", "mp"), None),
        check_vma=False,
    )
```

```python
import functools

import jax
import jax.numpy as jnp
from jax import lax
from jax.experimental import pallas as pl
from jax.experimental.pallas import tpu as pltpu
from jax.sharding import PartitionSpec as P

MESH = pl.DeviceIdType.MESH
LANES = 128
VMEM_GRANT = 60 * 2**20


def flip(index, mask, size):
    out, bit = index, 1
    while bit < size:
        if mask & bit:
            out = out + bit - 2 * bit * (lax.rem(lax.div(index, bit), 2))
        bit *= 2
    return out


def gelu(pre):
    return 0.5 * pre * (1.0 + lax.erf(pre * (0.5**0.5)))


def kernel(
    lines, tokens, gain, bias, w_in, b_in, w_out, b_out, out,
    shift, tok, win, wout, normed, hidden, part, own, from_y, sums, from_z, to_x, kept, from_x,
    tok_sem, win_sem, wout_sem, y_sem, z_sem, x_sem, local_sem, send_sem,
):
    dp, mp = lax.axis_index("dp"), lax.axis_index("mp")
    x, core = lax.div(dp, 2), lax.rem(dp, 2)
    z, y = lax.div(mp, 2), lax.rem(mp, 2)
    ox, oy = 1 - x, 1 - y
    rows, depth = tokens.shape[0], w_in.shape[0]
    units = w_in.shape[1]
    half = units // 2
    start = half // LANES * LANES
    width = units - start
    x_dev = (2 * ox + core, mp)
    core_dev = (2 * x + 1 - core, mp)
    y_dev = (dp, 2 * z + oy)
    z_at = [flip(z, k, lines) for k in range(lines)]
    z_dev = [(dp, 2 * z_at[k] + y) for k in range(lines)]

    barrier = pltpu.get_barrier_semaphore()
    partners = [x_dev, core_dev, y_dev] + z_dev[1:]
    for partner in partners:
        pl.semaphore_signal(barrier, inc=1, device_id=partner, device_id_type=MESH)
    pl.semaphore_wait(barrier, len(partners))

    sends = []

    def send(src, dst, sem, device):
        copy = pltpu.make_async_remote_copy(
            src_ref=src, dst_ref=dst, send_sem=send_sem.at[len(sends)], recv_sem=sem,
            device_id=device, device_id_type=MESH,
        )
        copy.start()
        sends.append(copy)

    def arrive(dst, sem):
        pltpu.make_async_remote_copy(
            src_ref=dst, dst_ref=dst, send_sem=send_sem.at[0], recv_sem=sem,
            device_id=x_dev, device_id_type=MESH,
        ).wait_recv()

    def slot(yy, zz, side):
        return (yy * lines + zz) * 2 + side

    mine = tok.at[slot(y, z, x)]
    mine_sem = tok_sem.at[y, z, x]
    send(tokens, mine, mine_sem, x_dev)
    for k in range(1, lines):
        send(tokens, mine, mine_sem, z_dev[k])
    send(tokens, mine, mine_sem, y_dev)
    locals_ = [pltpu.make_async_copy(tokens, mine, local_sem.at[0])]

    def columns(weight, side):
        return weight.at[:, pl.ds(pl.multiple_of(side * start, LANES), width)]


    def rows_of(full, owner):
        return full.at[pl.ds(pl.multiple_of(owner * depth, 16), depth), :]

    far, near, across = 2 * ox + core, 2 * x + 1 - core, 2 * ox + 1 - core
    send(columns(w_in, ox), rows_of(win, dp), win_sem.at[dp], x_dev)
    send(columns(w_in, x), rows_of(win, dp), win_sem.at[dp], core_dev)
    send(columns(w_out, ox), rows_of(wout, dp), wout_sem.at[dp], x_dev)
    send(columns(w_out, x), rows_of(wout, dp), wout_sem.at[dp], core_dev)
    locals_.append(pltpu.make_async_copy(columns(w_in, x), rows_of(win, dp), local_sem.at[1]))
    locals_.append(pltpu.make_async_copy(columns(w_out, x), rows_of(wout, dp), local_sem.at[2]))
    for copy in locals_:
        copy.start()

    shift[...] = jnp.broadcast_to(b_in[...], shift.shape)

    arrive(tok.at[slot(y, z, ox)], tok_sem.at[y, z, ox])
    for k in range(1, lines):
        send(tok.at[slot(y, z, ox)], tok.at[slot(y, z, ox)], tok_sem.at[y, z, ox], z_dev[k])
    send(tok.at[slot(y, z, ox)], tok.at[slot(y, z, ox)], tok_sem.at[y, z, ox], y_dev)
    for side in (x, ox):
        for k in range(1, lines):
            block, sem = tok.at[slot(y, z_at[k], side)], tok_sem.at[y, z_at[k], side]
            arrive(block, sem)
            send(block, block, sem, y_dev)

    def normalise(yy, zz):
        pair = jnp.concatenate(
            [tok[slot(yy, zz, 0)].astype(jnp.float32), tok[slot(yy, zz, 1)].astype(jnp.float32)], axis=0
        )
        center = jnp.mean(pair, axis=1, keepdims=True)
        spread = jnp.mean((pair - center) ** 2, axis=1, keepdims=True)
        value = (pair - center) / jnp.sqrt(spread + 1e-06) * gain[...] + bias[...]
        normed[yy, pl.ds(pl.multiple_of(zz * 2 * rows, 16), 2 * rows), :] = value.astype(
            normed.dtype
        )

    tile = 2 * LANES if width % (2 * LANES) == 0 else LANES

    def first(yy):
        def step(n, carry):
            at = pl.ds(pl.multiple_of(n * tile, LANES), tile)
            pre = jnp.dot(normed[yy], win[:, at], preferred_element_type=jnp.float32)
            pre = pre + shift[:1, pl.ds(pl.multiple_of(x * start + n * tile, LANES), tile)]
            unit = x * start + n * tile + lax.broadcasted_iota(jnp.int32, pre.shape, 1)
            keep = (unit >= x * half) & (unit < (x + 1) * half)
            hidden[yy, :, at] = jnp.where(keep, gelu(pre), 0.0).astype(hidden.dtype)
            return carry

        lax.fori_loop(0, width // tile, step, 0)

    def second(q, yy, zz):
        side = x if q == 0 else ox
        act = hidden[yy, pl.ds(pl.multiple_of(zz * 2 * rows, 16), 2 * rows), :]
        weight = wout[pl.ds(pl.multiple_of(side * 2 * depth, 16), 2 * depth), :]
        return lax.dot_general(
            act, weight, (((1,), (1,)), ((), ())), preferred_element_type=jnp.float32
        )

    def product(q):
        for k in range(lines):
            part[q, z_at[k]] = second(q, oy, z_at[k]).astype(part.dtype)
            send(part.at[q, z_at[k]], from_y.at[q, z_at[k]], y_sem.at[q, z_at[k]], y_dev)

    def product_own(q):
        def step(zz, carry):
            own[q, zz] = second(q, y, zz)
            return carry

        lax.fori_loop(0, lines, step, 0)

    locals_[0].wait()

    def norm_own(zz, carry):
        normalise(y, zz)
        return carry

    lax.fori_loop(0, lines, norm_own, 0)

    arrive(rows_of(win, far), win_sem.at[far])
    send(rows_of(win, far), rows_of(win, far), win_sem.at[far], core_dev)
    locals_[1].wait()
    arrive(rows_of(win, near), win_sem.at[near])
    arrive(rows_of(win, across), win_sem.at[across])
    first(y)
    locals_[2].wait()
    arrive(rows_of(wout, near), wout_sem.at[near])
    product_own(0)

    for k in range(lines):
        for side in (x, ox):
            arrive(tok.at[slot(oy, z_at[k], side)], tok_sem.at[oy, z_at[k], side])
        normalise(oy, z_at[k])
    first(oy)

    def along_z(q):
        for k in list(range(1, lines)) + [0]:
            at = z_at[k]
            arrive(from_y.at[q, at], y_sem.at[q, at])
            total = own[q, at] + from_y[q, at].astype(jnp.float32)
            if k:
                sums[q, at] = total.astype(sums.dtype)
                send(sums.at[q, at], from_z.at[q, z], z_sem.at[q, z], z_dev[k])
            else:
                own[q, at] = total

    def along_x(q):
        side = x if q == 0 else ox
        total = own[q, z]
        for k in range(1, lines):
            arrive(from_z.at[q, z_at[k]], z_sem.at[q, z_at[k]])
            total = total + from_z[q, z_at[k]].astype(jnp.float32)
        own[q, z] = total
        to_x[q] = own[q, z, pl.ds(pl.multiple_of(ox * rows, 8), rows), :].astype(to_x.dtype)
        send(to_x.at[q], from_x.at[side], x_sem.at[side], x_dev)
        kept[side] = own[q, z, pl.ds(pl.multiple_of(x * rows, 8), rows), :]

    product(0)
    arrive(rows_of(wout, far), wout_sem.at[far])
    send(rows_of(wout, far), rows_of(wout, far), wout_sem.at[far], core_dev)
    along_z(0)
    arrive(rows_of(wout, across), wout_sem.at[across])
    product(1)
    product_own(1)
    along_x(0)
    along_z(1)
    along_x(1)
    columns_of, added = 2 * depth, b_out[...]
    for side in range(2):
        at = slice(side * columns_of, (side + 1) * columns_of)
        arrive(from_x.at[side], x_sem.at[side])
        total = kept[side] + from_x[side].astype(jnp.float32)
        out[:, at] = tok[slot(y, z, x), :, at].astype(jnp.float32) + total + added[:, at]
    for copy in sends:
        copy.wait_send()


def fused(mp, tokens, gain, bias, w_in, b_in, w_out, b_out):
    rows, dim = tokens.shape
    depth, units = w_in.shape
    lines = mp // 2
    width = units - units // 2 // LANES * LANES
    columns = 2 * depth
    bf16, f32, dma = jnp.bfloat16, jnp.float32, pltpu.SemaphoreType.DMA
    vmem = pl.BlockSpec(memory_space=pltpu.VMEM)
    hbm = pl.BlockSpec(memory_space=pl.ANY)
    n_sends = (lines + 1) * 2 + 4 + 2 * (lines - 1) + 2 + 2 * (lines + lines - 1 + 1)
    return pl.pallas_call(
        functools.partial(kernel, lines),
        out_shape=jax.ShapeDtypeStruct((rows, dim), f32),
        in_specs=[hbm, vmem, vmem, hbm, vmem, hbm, vmem],
        out_specs=vmem,
        scratch_shapes=[
            pltpu.VMEM((8, units), f32),
            pltpu.VMEM((4 * lines + 1, rows, dim), bf16),
            pltpu.VMEM((dim, width), bf16),
            pltpu.VMEM((dim, width), bf16),
            pltpu.VMEM((2, lines * 2 * rows, dim), bf16),
            pltpu.VMEM((2, lines * 2 * rows, width), bf16),
            pltpu.VMEM((2, lines, 2 * rows, columns), bf16),
            pltpu.VMEM((2, lines, 2 * rows, columns), f32),
            pltpu.VMEM((2, lines, 2 * rows, columns), bf16),
            pltpu.VMEM((2, lines, 2 * rows, columns), bf16),
            pltpu.VMEM((2, lines, 2 * rows, columns), bf16),
            pltpu.VMEM((3, rows, columns), bf16),
            pltpu.VMEM((2, rows, columns), f32),
            pltpu.VMEM((3, rows, columns), bf16),
            dma((2, lines, 2)),
            dma((4,)),
            dma((4,)),
            dma((2, lines)),
            dma((2, lines)),
            dma((2,)),
            dma((3,)),
            dma((n_sends,)),
        ],
        compiler_params=pltpu.CompilerParams(
            collective_id=0, has_side_effects=True, vmem_limit_bytes=VMEM_GRANT
        ),
    )(tokens, gain[None], bias[None], w_in, b_in[None], w_out.T, b_out[None]).astype(bf16)


def gathered(tokens, norm_gain, norm_bias, w_in, b_in, w_out, b_out):
    values = tokens.astype(jnp.float32)
    center = jnp.mean(values, axis=1, keepdims=True)
    spread = jnp.mean((values - center) ** 2, axis=1, keepdims=True)
    normed = ((values - center) / jnp.sqrt(spread + 1e-06) * norm_gain + norm_bias).astype(
        jnp.bfloat16
    )
    w_in_full = lax.all_gather(w_in, "dp", axis=0, tiled=True)
    everyone = lax.all_gather(normed, "mp", axis=0, tiled=True)
    pre = jnp.dot(everyone, w_in_full, preferred_element_type=jnp.float32) + b_in
    hidden = jax.nn.gelu(pre, approximate=False).astype(jnp.bfloat16)
    w_out_full = lax.all_gather(w_out, "dp", axis=1, tiled=True)
    summed = lax.psum_scatter(
        jnp.dot(hidden, w_out_full, preferred_element_type=jnp.float32),
        "mp",
        scatter_dimension=0,
        tiled=True,
    )
    return (values + summed + b_out).astype(jnp.bfloat16)


def on_device(dp, mp, tokens, norm_gain, norm_bias, w_in, b_in, w_out, b_out):
    rows, (depth, units) = tokens.shape[0], w_in.shape
    fits = (
        dp == 4
        and mp % 2 == 0
        and mp & (mp - 1) == 0
        and units % LANES == 0
        and depth % 16 == 0
        and 2 * depth % LANES == 0
        and rows % 8 == 0
        and mp * 2 * rows * (2 * depth) * 2 * 24 < VMEM_GRANT
    )
    if fits:
        return fused(mp, tokens, norm_gain, norm_bias, w_in, b_in, w_out, b_out)
    return gathered(tokens, norm_gain, norm_bias, w_in, b_in, w_out, b_out)


def solution(mesh):
    placed = (P(("dp", "mp"), None), P(), P(), P("dp", "mp"), P("mp"), P("mp", "dp"), P())
    return jax.shard_map(
        functools.partial(on_device, mesh.shape["dp"], mesh.shape["mp"]),
        mesh=mesh,
        in_specs=placed,
        out_specs=P(("dp", "mp"), None),
        check_vma=False,
    )
```
